64 devices in a mesh: dp: 8 (over x, y, core), tp: 8 (over z).
Axes of the slice: x: 2, y: 2, z: 8, core: 2. Of those that a mesh axis runs over, the one named last changes fastest.
The devices are a block of a 4x4x8 slice.
Arguments:
- x: bfloat16 [10240, 7168], P(('dp', 'tp')), parts along dimension 0
- w_gate: bfloat16 [7168, 18432], P(None, 'tp')
- w_up: bfloat16 [7168, 18432], P(None, 'tp')
- w_down: bfloat16 [18432, 7168], P('tp')
Outputs:
- output: bfloat16 [10240, 7168], P(('dp', 'tp')), parts along dimension 0
There are 8 independent parts. The reference program is written for one: setup_inputs(seed, part) draws one part's arguments, and reference() takes and returns one part's arrays. A program takes and returns all parts, laid end to end along the dimension named above; an argument that names none is the same for every part.
All inputs are finite; a program needn't handle non-finite values.
Results may differ from the reference program's by a relative error of at most 0.016.
Values are sent between devices in bfloat16 or wider.
A program may use at most 768 MiB of HBM per device.

```python
import jax
import jax.numpy as jnp

ROWS = 1280
D = 7168
FF = 18432


def setup_inputs(seed: int = 0, part: int = 0) -> dict:
    kx, kg, ku, kd = jax.random.split(jax.random.key(seed), 4)
    drawn = {
        "x": jax.random.normal(jax.random.fold_in(kx, part), (ROWS, D), jnp.float32),
        "w_gate": jax.random.normal(kg, (D, FF), jnp.float32) * D**-0.5,
        "w_up": jax.random.normal(ku, (D, FF), jnp.float32) * D**-0.5,
        "w_down": jax.random.normal(kd, (FF, D), jnp.float32) * FF**-0.5,
    }
    return {k: v.astype(jnp.bfloat16) for k, v in drawn.items()}


def reference(x, w_gate, w_up, w_down):
    gate = jnp.dot(x, w_gate, preferred_element_type=jnp.float32)
    up = jnp.dot(x, w_up, preferred_element_type=jnp.float32)
    hidden = (jax.nn.silu(gate) * up).astype(jnp.bfloat16)
    return jnp.dot(hidden, w_down, preferred_element_type=jnp.float32).astype(jnp.bfloat16)
```

```python
import jax
import jax.numpy as jnp
from jax import lax
from jax.sharding import PartitionSpec as P


def solution(mesh):
    def block(x, w_gate, w_up, w_down):
        rows = lax.all_gather(x, "tp", axis=0, tiled=True)
        gate = jnp.dot(rows, w_gate, preferred_element_type=jnp.float32)
        up = jnp.dot(rows, w_up, preferred_element_type=jnp.float32)
        hidden = (jax.nn.silu(gate) * up).astype(jnp.bfloat16)
        term = jnp.dot(hidden, w_down, preferred_element_type=jnp.float32).astype(jnp.bfloat16)
        return lax.psum_scatter(term, "tp", scatter_dimension=0, tiled=True)

    def step(x, w_gate, w_up, w_down):
        half = x.shape[0] // 2
        parts = [block(part, w_gate, w_up, w_down) for part in (x[:half], x[half:])]
        return jnp.concatenate(parts, axis=0)

    return jax.shard_map(
        step,
        mesh=mesh,
        in_specs=(P(("dp", "tp"), None), P(None, "tp"), P(None, "tp"), P("tp", None)),
        out_specs=P(("dp", "tp"), None),
        check_vma=False,
    )
```

```python
import functools

import jax
import jax.numpy as jnp
from jax import lax
from jax.experimental import pallas as pl
from jax.experimental.pallas import tpu as pltpu
from jax.sharding import PartitionSpec as P

MESH = pl.DeviceIdType.MESH
PIECES = 5
STRIPS = 7
LANES = 128
WIDE = 256
DELAY = 2


def kernel(
    n, x_ref, wg_ref, wu_ref, wd_ref, y_ref,
    xg, hid, terms, wbuf, slots, stage, own,
    x_sem, w_sem, ag_send, ag_recv, head_send, rs_send, rs_recv, y_sem,
):
    me = lax.axis_index("tp")
    peer = (lax.rem(me + 1, n), lax.rem(me + n - 1, n))
    rows, depth = x_ref.shape
    ff = wg_ref.shape[1]
    half = rows // 2
    group = n * half
    piece, strip = half // PIECES, depth // STRIPS
    far, near = n // 2, n - 1 - n // 2
    hops = ((far, near), (near, far))
    up_tiles, down_tiles = ff // LANES, depth // (2 * WIDE)
    per_strip = down_tiles // STRIPS

    def at(offset):
        return lax.rem(me + offset + 2 * n, n)

    def upstream(way, k):
        return at(-k) if way == 0 else at(k)

    def downstream(way, k):
        return at(k) if way == 0 else at(-k)


    def gather_copy(h, way, chunk, p, a):
        span = pl.ds(pl.multiple_of(h * group + chunk * half + p * piece, piece), piece)
        index = a if h == 0 else a + hops[0][way] * PIECES
        return pltpu.make_async_remote_copy(
            src_ref=xg.at[span],
            dst_ref=xg.at[span],
            send_sem=ag_send.at[h, way],
            recv_sem=ag_recv.at[way, index],
            device_id={"tp": peer[way]},
            device_id_type=MESH,
        )

    def gather_own(h, way):
        def send(p, _):
            gather_copy(h, way, me, p, p).start()
            return 0

        lax.fori_loop(0, PIECES, send, 0)

    def gather_event(h, way, a, forward):
        hop = lax.div(a, PIECES)
        p = a - hop * PIECES
        chunk = upstream(way, hop + 1)
        gather_copy(h, way, chunk, p, a).wait_recv()
        if forward:
            gather_copy(h, way, chunk, p, a + PIECES).start()

    def gather_sent(h, way):
        span = pl.ds(0, hops[h][way] * half)
        pltpu.make_async_remote_copy(
            src_ref=xg.at[span],
            dst_ref=xg.at[span],
            send_sem=ag_send.at[h, way],
            recv_sem=ag_recv.at[way, 0],
            device_id={"tp": peer[way]},
            device_id_type=MESH,
        ).wait_send()


    def columns(p):
        return pl.ds(pl.multiple_of(p * strip, LANES), strip)

    def of_device(d):
        return pl.ds(pl.multiple_of(d * half, 16), half)

    def box(h, way, k, p):
        first = 0 if way == 0 else hops[h][0]
        span = pl.ds(pl.multiple_of((first + k - 1) * half, 16), half)
        return (slots if h == 0 else xg).at[span, columns(p)]

    def sum_copy(h, way, k, p, src, send_sem):
        return pltpu.make_async_remote_copy(
            src_ref=src,
            dst_ref=box(h, way, k, p),
            send_sem=send_sem,
            recv_sem=rs_recv.at[h, way, (k - 1) * STRIPS + p],
            device_id={"tp": peer[way]},
            device_id_type=MESH,
        )

    def sum_wait(h, way, k, p):
        arrived = box(h, way, k, p)
        sum_copy(h, way, k, p, arrived, rs_send.at[h, way]).wait_recv()
        return arrived

    def sum_head(h, p):
        for way in range(2):
            target = downstream(way, hops[h][way])
            held = stage.at[pl.ds(way * half, half), columns(p)]
            held[...] = terms[of_device(target), columns(p)].astype(jnp.bfloat16)
            sum_copy(h, way, 1, p, held, head_send.at[h, way]).start()

    def sum_event(h, way, e):
        hop = lax.div(e, STRIPS)
        p = e - hop * STRIPS
        arrived = sum_wait(h, way, hop + 1, p)
        target = downstream(way, hops[h][way] - 1 - hop)
        term = terms[of_device(target), columns(p)]
        arrived[...] = (arrived[...].astype(jnp.float32) + term).astype(jnp.bfloat16)
        sum_copy(h, way, hop + 2, p, arrived, rs_send.at[h, way]).start()

    def sums_sent(sem, ref, count):
        span = pl.ds(0, count)
        pltpu.make_async_remote_copy(
            src_ref=ref.at[span],
            dst_ref=ref.at[span],
            send_sem=sem,
            recv_sem=rs_recv.at[0, 0, 0],
            device_id={"tp": peer[0]},
            device_id_type=MESH,
        ).wait_send()

    def finish(h, p, done):
        pltpu.make_async_copy(
            done, y_ref.at[pl.ds(h * half, half), columns(p)], y_sem.at[h]
        ).start()


    def up_copies(i, s):
        span = pl.ds(pl.multiple_of(i * LANES, LANES), LANES)
        return [
            pltpu.make_async_copy(
                ref.at[:, span], wbuf.at[s, :, pl.ds(b * LANES, LANES)], w_sem.at[s, b]
            )
            for b, ref in enumerate((wg_ref, wu_ref))
        ]

    def down_copies(j, s):
        copies = []
        for b in range(2):
            span = pl.ds(pl.multiple_of((2 * j + b) * WIDE, WIDE), WIDE)
            copies.append(
                pltpu.make_async_copy(
                    wd_ref.at[:, span], wbuf.at[s, pl.ds(b * ff, ff)], w_sem.at[s, b]
                )
            )
        return copies

    def start(copies):
        for copy in copies:
            copy.start()

    def wait(copies):
        for copy in copies:
            copy.wait()

    def gate_up(h, first, events):
        def tile(i, _):
            s = lax.rem(first + i, 2)

            @pl.when(i + 1 < up_tiles)
            def _():
                start(up_copies(i + 1, 1 - s))

            @pl.when(i + 1 == up_tiles)
            def _():
                start(down_copies(0, 1 - s))

            wait(up_copies(i, s))
            both = jnp.dot(
                xg[h * group : (h + 1) * group, :],
                wbuf[s],
                preferred_element_type=jnp.float32,
            )
            gate, up = both[:, :LANES], both[:, LANES:]
            span = pl.ds(pl.multiple_of(i * LANES, LANES), LANES)
            hid[:, span] = (jax.nn.silu(gate) * up).astype(jnp.bfloat16)
            events(i)
            return 0

        lax.fori_loop(0, up_tiles, tile, 0)

    def down(h, first, before, after):
        def one_strip(p, _):
            before(p)

            def tile(t, _):
                j = p * per_strip + t
                s = lax.rem(first + j, 2)

                @pl.when(j + 1 < down_tiles)
                def _():
                    start(down_copies(j + 1, 1 - s))

                if h == 0:

                    @pl.when(j + 1 == down_tiles)
                    def _():
                        start(up_copies(0, 1 - s))

                wait(down_copies(j, s))
                for b in range(2):
                    span = pl.ds(pl.multiple_of((2 * j + b) * WIDE, WIDE), WIDE)
                    terms[:, span] = jnp.dot(
                        hid[...],
                        wbuf[s, b * ff : (b + 1) * ff, :],
                        preferred_element_type=jnp.float32,
                    )
                return 0

            lax.fori_loop(0, per_strip, tile, 0)
            after(p)
            return 0

        lax.fori_loop(0, STRIPS, one_strip, 0)

    def spread(i, tiles, delay, count, event):
        def upto(t):
            return lax.div(jnp.maximum(t - delay, 0) * count, tiles - delay)

        def run(e, _):
            event(e)
            return 0

        lax.fori_loop(upto(i), upto(i + 1), run, 0)

    def loop(lo, hi, event):
        def run(e, _):
            event(e)
            return 0

        lax.fori_loop(lo, hi, run, 0)


    own_copies = [
        pltpu.make_async_copy(
            x_ref.at[pl.ds(h * half, half)],
            xg.at[pl.ds(pl.multiple_of(h * group + me * half, 16), half)],
            x_sem.at[h],
        )
        for h in range(2)
    ]
    start(own_copies)

    barrier = pltpu.get_barrier_semaphore()
    for other in peer:
        pl.semaphore_signal(barrier, inc=1, device_id={"tp": other}, device_id_type=MESH)
    pl.semaphore_wait(barrier, 2)

    own_copies[0].wait()
    gather_own(0, 0)
    gather_own(0, 1)
    start(up_copies(0, 0))
    own_copies[1].wait()

    def both_on(a):
        gather_event(0, 0, a, True)
        gather_event(0, 1, a, True)

    loop(0, (near - 1) * PIECES, both_on)
    gather_own(1, 1)

    def one_on(a):
        gather_event(0, 0, a, True)
        gather_event(0, 1, a, False)

    loop((near - 1) * PIECES, near * PIECES, one_on)
    gather_own(1, 0)

    def last_of_first(a):
        gather_event(0, 0, a, False)
        gather_event(1, 1, a - near * PIECES, True)

    loop(near * PIECES, far * PIECES, last_of_first)

    def second_on(j):
        gather_event(1, 0, j, True)
        gather_event(1, 1, j + PIECES, True)

    gate_up(
        0, 0,
        lambda i: spread(i, up_tiles, 0, (near - 1) * PIECES, second_on),
    )
    gather_sent(0, 0)
    gather_sent(0, 1)
    down(0, up_tiles, lambda p: None, lambda p: sum_head(0, p))

    def second_in(j):
        gather_event(1, 0, j, False)
        gather_event(1, 1, j + PIECES, False)

    loop((near - 1) * PIECES, near * PIECES, second_in)

    def first_sums(e):
        sum_event(0, 0, e)
        sum_event(0, 1, e)

    gate_up(
        1, up_tiles + down_tiles,
        lambda i: spread(i, up_tiles, min(DELAY, up_tiles - 1), (near - 1) * STRIPS, first_sums),
    )
    for way in range(2):
        sums_sent(head_send.at[0, way], stage, half)

    def near_end(p):
        sum_event(0, 0, (near - 1) * STRIPS + p)
        arrived = sum_wait(0, 1, near, p)
        own[:, columns(p)] = arrived[...].astype(jnp.float32) + terms[of_device(me), columns(p)]

    down(1, 2 * up_tiles + down_tiles, near_end, lambda p: sum_head(1, p))

    def first_end(p):
        arrived = sum_wait(0, 0, far, p)
        total = arrived[...].astype(jnp.float32) + own[:, columns(p)]
        arrived[...] = total.astype(jnp.bfloat16)
        finish(0, p, arrived)
        sum_event(1, 1, p)

    loop(0, STRIPS, first_end)

    def second_sums(e):
        sum_event(1, 1, e + STRIPS)
        sum_event(1, 0, e)

    loop(0, (near - 1) * STRIPS, second_sums)

    def second_end(p):
        one, other = sum_wait(1, 0, near, p), sum_wait(1, 1, far, p)
        total = one[...].astype(jnp.float32) + other[...].astype(jnp.float32)
        one[...] = (total + terms[of_device(me), columns(p)]).astype(jnp.bfloat16)
        finish(1, p, one)

    loop(0, STRIPS, second_end)

    for way in range(2):
        gather_sent(1, way)
        sums_sent(head_send.at[1, way], stage, half)
        for h in range(2):
            sums_sent(rs_send.at[h, way], slots, (hops[h][way] - 1) * half)
    for h in range(2):
        span = pl.ds(h * half, half)
        pltpu.make_async_copy(slots.at[pl.ds(0, half)], y_ref.at[span], y_sem.at[h]).wait()


def solution(mesh):
    n = mesh.shape["tp"]

    def step(x, w_gate, w_up, w_down):
        rows, depth = x.shape
        ff = w_gate.shape[1]
        half = rows // 2
        far = n // 2
        bf16, f32 = jnp.bfloat16, jnp.float32
        dma = pltpu.SemaphoreType.DMA
        return pl.pallas_call(
            functools.partial(kernel, n),
            name="mlp_ring",
            out_shape=jax.ShapeDtypeStruct((rows, depth), x.dtype),
            in_specs=[pl.BlockSpec(memory_space=pl.ANY)] * 4,
            out_specs=pl.BlockSpec(memory_space=pl.ANY),
            scratch_shapes=[
                pltpu.VMEM((n * rows, depth), bf16),
                pltpu.VMEM((n * half, ff), bf16),
                pltpu.VMEM((n * half, depth), f32),
                pltpu.VMEM((2, depth, WIDE), bf16),
                pltpu.VMEM(((n - 1) * half, depth), bf16),
                pltpu.VMEM((2 * half, depth), bf16),
                pltpu.VMEM((half, depth), f32),
                dma((2,)),
                dma((2, 2)),
                dma((2, 2)),
                dma((2, (n - 1) * PIECES)),
                dma((2, 2)),
                dma((2, 2)),
                dma((2, 2, far * STRIPS)),
                dma((2,)),
            ],
            compiler_params=pltpu.CompilerParams(
                collective_id=0, has_side_effects=True, vmem_limit_bytes=67043328
            ),
        )(x, w_gate, w_up, w_down)

    return jax.shard_map(
        step,
        mesh=mesh,
        in_specs=(P(("dp", "tp"), None), P(None, "tp"), P(None, "tp"), P("tp", None)),
        out_specs=P(("dp", "tp"), None),
        check_vma=False,
    )
```

```python
import functools

import jax
import jax.numpy as jnp
from jax import lax
from jax.experimental import pallas as pl
from jax.experimental.pallas import tpu as pltpu
from jax.sharding import PartitionSpec as P

MESH = pl.DeviceIdType.MESH
PIECES = 5
STRIPS = 7
LANES = 128
WIDE = 256
VMEM_GRANT = 63000 * 1024
DELAY = 2


def kernel(
    n, x_ref, wg_ref, wu_ref, wd_ref, y_ref,
    xg, hid, terms, wbuf, slots, stage, own,
    x_sem, w_sem, ag_send, ag_recv, head_send, rs_send, rs_recv,
):
    me = lax.axis_index("tp")
    peer = (lax.rem(me + 1, n), lax.rem(me + n - 1, n))
    rows, depth = x_ref.shape
    ff = wg_ref.shape[1]
    half = rows // 2
    group = n * half
    piece, strip = half // PIECES, depth // STRIPS
    far, near = n // 2, n - 1 - n // 2
    hops = ((far, near), (near, far))
    up_tiles, down_tiles = ff // LANES, depth // (2 * WIDE)
    per_strip = down_tiles // STRIPS

    def at(offset):
        return lax.rem(me + offset + 2 * n, n)

    def upstream(way, k):
        return at(-k) if way == 0 else at(k)

    def downstream(way, k):
        return at(k) if way == 0 else at(-k)


    def gather_copy(h, way, chunk, p, a):
        span = pl.ds(pl.multiple_of(h * group + chunk * half + p * piece, piece), piece)
        index = a if h == 0 else a + hops[0][way] * PIECES
        return pltpu.make_async_remote_copy(
            src_ref=xg.at[span],
            dst_ref=xg.at[span],
            send_sem=ag_send.at[h, way],
            recv_sem=ag_recv.at[way, index],
            device_id={"tp": peer[way]},
            device_id_type=MESH,
        )

    def gather_own(h, way):
        def send(p, _):
            gather_copy(h, way, me, p, p).start()
            return 0

        lax.fori_loop(0, PIECES, send, 0)

    def gather_event(h, way, a, forward):
        hop = lax.div(a, PIECES)
        p = a - hop * PIECES
        chunk = upstream(way, hop + 1)
        gather_copy(h, way, chunk, p, a).wait_recv()
        if forward:
            gather_copy(h, way, chunk, p, a + PIECES).start()

    def gather_sent(h, way):
        span = pl.ds(0, hops[h][way] * half)
        pltpu.make_async_remote_copy(
            src_ref=xg.at[span],
            dst_ref=xg.at[span],
            send_sem=ag_send.at[h, way],
            recv_sem=ag_recv.at[way, 0],
            device_id={"tp": peer[way]},
            device_id_type=MESH,
        ).wait_send()


    def columns(p):
        return pl.ds(pl.multiple_of(p * strip, LANES), strip)

    def of_device(d):
        return pl.ds(pl.multiple_of(d * half, 16), half)

    def box(h, way, k, p):
        first = 0 if way == 0 else hops[h][0]
        span = pl.ds(pl.multiple_of((first + k - 1) * half, 16), half)
        return (slots if h == 0 else xg).at[span, columns(p)]

    def sum_copy(h, way, k, p, src, send_sem):
        return pltpu.make_async_remote_copy(
            src_ref=src,
            dst_ref=box(h, way, k, p),
            send_sem=send_sem,
            recv_sem=rs_recv.at[h, way, (k - 1) * STRIPS + p],
            device_id={"tp": peer[way]},
            device_id_type=MESH,
        )

    def sum_wait(h, way, k, p):
        arrived = box(h, way, k, p)
        sum_copy(h, way, k, p, arrived, rs_send.at[h, way]).wait_recv()
        return arrived

    def sum_head(h, p):
        for way in range(2):
            target = downstream(way, hops[h][way])
            held = stage.at[pl.ds(way * half, half), columns(p)]
            held[...] = terms[of_device(target), columns(p)].astype(jnp.bfloat16)
            sum_copy(h, way, 1, p, held, head_send.at[h, way]).start()

    def sum_event(h, way, e):
        hop = lax.div(e, STRIPS)
        p = e - hop * STRIPS
        arrived = sum_wait(h, way, hop + 1, p)
        target = downstream(way, hops[h][way] - 1 - hop)
        term = terms[of_device(target), columns(p)]
        arrived[...] = (arrived[...].astype(jnp.float32) + term).astype(jnp.bfloat16)
        sum_copy(h, way, hop + 2, p, arrived, rs_send.at[h, way]).start()

    def sums_sent(sem, ref, count):
        span = pl.ds(0, count)
        pltpu.make_async_remote_copy(
            src_ref=ref.at[span],
            dst_ref=ref.at[span],
            send_sem=sem,
            recv_sem=rs_recv.at[0, 0, 0],
            device_id={"tp": peer[0]},
            device_id_type=MESH,
        ).wait_send()


    def up_copies(i, s):
        span = pl.ds(pl.multiple_of(i * LANES, LANES), LANES)
        return [
            pltpu.make_async_copy(
                ref.at[:, span], wbuf.at[s, :, pl.ds(b * LANES, LANES)], w_sem.at[s, b]
            )
            for b, ref in enumerate((wg_ref, wu_ref))
        ]

    def down_copies(j, s):
        copies = []
        for b in range(2):
            span = pl.ds(pl.multiple_of((2 * j + b) * WIDE, WIDE), WIDE)
            copies.append(
                pltpu.make_async_copy(
                    wd_ref.at[:, span], wbuf.at[s, pl.ds(b * ff, ff)], w_sem.at[s, b]
                )
            )
        return copies

    def start(copies):
        for copy in copies:
            copy.start()

    def wait(copies):
        for copy in copies:
            copy.wait()

    def gate_up(h, first, events):
        def tile(i, _):
            s = lax.rem(first + i, 2)

            @pl.when(i + 1 < up_tiles)
            def _():
                start(up_copies(i + 1, 1 - s))

            @pl.when(i + 1 == up_tiles)
            def _():
                start(down_copies(0, 1 - s))

            wait(up_copies(i, s))
            both = jnp.dot(
                xg[h * group : (h + 1) * group, :],
                wbuf[s],
                preferred_element_type=jnp.float32,
            )
            gate, up = both[:, :LANES], both[:, LANES:]
            span = pl.ds(pl.multiple_of(i * LANES, LANES), LANES)
            hid[:, span] = (jax.nn.silu(gate) * up).astype(jnp.bfloat16)
            events(i)
            return 0

        lax.fori_loop(0, up_tiles, tile, 0)

    def down(h, first, before, after):
        def one_strip(p, _):
            before(p)

            def tile(t, _):
                j = p * per_strip + t
                s = lax.rem(first + j, 2)

                @pl.when(j + 1 < down_tiles)
                def _():
                    start(down_copies(j + 1, 1 - s))

                if h == 0:

                    @pl.when(j + 1 == down_tiles)
                    def _():
                        start(up_copies(0, 1 - s))

                wait(down_copies(j, s))
                for b in range(2):
                    span = pl.ds(pl.multiple_of((2 * j + b) * WIDE, WIDE), WIDE)
                    terms[:, span] = jnp.dot(
                        hid[...],
                        wbuf[s, b * ff : (b + 1) * ff, :],
                        preferred_element_type=jnp.float32,
                    )
                return 0

            lax.fori_loop(0, per_strip, tile, 0)
            after(p)
            return 0

        lax.fori_loop(0, STRIPS, one_strip, 0)

    def spread(i, tiles, delay, count, event):
        def upto(t):
            return lax.div(jnp.maximum(t - delay, 0) * count, tiles - delay)

        def run(e, _):
            event(e)
            return 0

        lax.fori_loop(upto(i), upto(i + 1), run, 0)

    def loop(lo, hi, event):
        def run(e, _):
            event(e)
            return 0

        lax.fori_loop(lo, hi, run, 0)


    own_copies = [
        pltpu.make_async_copy(
            x_ref.at[pl.ds(h * half, half)],
            xg.at[pl.ds(pl.multiple_of(h * group + me * half, 16), half)],
            x_sem.at[h],
        )
        for h in range(2)
    ]
    own_copies[0].start()

    barrier = pltpu.get_barrier_semaphore()
    for other in peer:
        pl.semaphore_signal(barrier, inc=1, device_id={"tp": other}, device_id_type=MESH)
    pl.semaphore_wait(barrier, 2)

    own_copies[0].wait()
    gather_own(0, 0)
    gather_own(0, 1)
    own_copies[1].start()
    start(up_copies(0, 0))
    own_copies[1].wait()

    def both_on(a):
        gather_event(0, 0, a, True)
        gather_event(0, 1, a, True)

    loop(0, (near - 1) * PIECES, both_on)
    gather_own(1, 1)

    def one_on(a):
        gather_event(0, 0, a, True)
        gather_event(0, 1, a, False)

    loop((near - 1) * PIECES, near * PIECES, one_on)
    gather_own(1, 0)

    def last_of_first(a):
        gather_event(0, 0, a, False)
        gather_event(1, 1, a - near * PIECES, True)

    loop(near * PIECES, far * PIECES, last_of_first)

    def second_on(j):
        gather_event(1, 0, j, True)
        gather_event(1, 1, j + PIECES, True)

    gate_up(
        0, 0,
        lambda i: spread(i, up_tiles, 0, (near - 1) * PIECES, second_on),
    )
    gather_sent(0, 0)
    gather_sent(0, 1)
    down(0, up_tiles, lambda p: None, lambda p: sum_head(0, p))

    def second_in(j):
        gather_event(1, 0, j, False)
        gather_event(1, 1, j + PIECES, False)

    loop((near - 1) * PIECES, near * PIECES, second_in)

    def first_sums(e):
        sum_event(0, 0, e)
        sum_event(0, 1, e)

    gate_up(
        1, up_tiles + down_tiles,
        lambda i: spread(i, up_tiles, min(DELAY, up_tiles - 1), (near - 1) * STRIPS, first_sums),
    )
    for way in range(2):
        sums_sent(head_send.at[0, way], stage, half)

    def near_end(p):
        sum_event(0, 0, (near - 1) * STRIPS + p)
        arrived = sum_wait(0, 1, near, p)
        own[:, columns(p)] = arrived[...].astype(jnp.float32) + terms[of_device(me), columns(p)]

    down(1, 2 * up_tiles + down_tiles, near_end, lambda p: sum_head(1, p))

    def first_end(p):
        arrived = sum_wait(0, 0, far, p)
        total = arrived[...].astype(jnp.float32) + own[:, columns(p)]
        y_ref[pl.ds(0, half), columns(p)] = total.astype(jnp.bfloat16)
        sum_event(1, 1, p)

    loop(0, STRIPS, first_end)

    def second_sums(e):
        sum_event(1, 1, e + STRIPS)
        sum_event(1, 0, e)

    loop(0, (near - 1) * STRIPS, second_sums)

    def second_end(p):
        one, other = sum_wait(1, 0, near, p), sum_wait(1, 1, far, p)
        total = one[...].astype(jnp.float32) + other[...].astype(jnp.float32)
        total += terms[of_device(me), columns(p)]
        y_ref[pl.ds(half, half), columns(p)] = total.astype(jnp.bfloat16)

    loop(0, STRIPS, second_end)

    for way in range(2):
        gather_sent(1, way)
        sums_sent(head_send.at[1, way], stage, half)
        for h in range(2):
            sums_sent(rs_send.at[h, way], slots, (hops[h][way] - 1) * half)


def solution(mesh):
    n = mesh.shape["tp"]

    def step(x, w_gate, w_up, w_down):
        rows, depth = x.shape
        ff = w_gate.shape[1]
        half = rows // 2
        far = n // 2
        bf16, f32 = jnp.bfloat16, jnp.float32
        dma = pltpu.SemaphoreType.DMA
        return pl.pallas_call(
            functools.partial(kernel, n),
            name="mlp_ring",
            out_shape=pltpu.VMEM((rows, depth), x.dtype),
            in_specs=[pl.BlockSpec(memory_space=pl.ANY)] * 4,
            out_specs=pl.BlockSpec(memory_space=pltpu.VMEM),
            scratch_shapes=[
                pltpu.VMEM((n * rows, depth), bf16),
                pltpu.VMEM((n * half, ff), bf16),
                pltpu.VMEM((n * half, depth), f32),
                pltpu.VMEM((2, depth, WIDE), bf16),
                pltpu.VMEM(((n - 1) * half, depth), bf16),
                pltpu.VMEM((2 * half, depth), bf16),
                pltpu.VMEM((half, depth), f32),
                dma((2,)),
                dma((2, 2)),
                dma((2, 2)),
                dma((2, (n - 1) * PIECES)),
                dma((2, 2)),
                dma((2, 2)),
                dma((2, 2, far * STRIPS)),
            ],
            compiler_params=pltpu.CompilerParams(
                collective_id=0, has_side_effects=True, vmem_limit_bytes=VMEM_GRANT
            ),
        )(x, w_gate, w_up, w_down)

    return jax.shard_map(
        step,
        mesh=mesh,
        in_specs=(P(("dp", "tp"), None), P(None, "tp"), P(None, "tp"), P("tp", None)),
        out_specs=P(("dp", "tp"), None),
        check_vma=False,
    )
```

```python
import functools

import jax
import jax.numpy as jnp
from jax import lax
from jax.experimental import pallas as pl
from jax.experimental.pallas import tpu as pltpu
from jax.sharding import PartitionSpec as P

MESH = pl.DeviceIdType.MESH
PIECES = 2
STRIPS = 2
LANES = 128
WIDE = 256
VMEM_GRANT = 63000 * 1024
DELAY = 2


def kernel(
    n, x_ref, wg_ref, wu_ref, wd_ref, y_ref,
    xg, hid, terms, wbuf, slots, stage, own,
    x_sem, w_sem, ag_send, ag_recv, head_send, rs_send, rs_recv,
):
    me = lax.axis_index("tp")
    peer = (lax.rem(me + 1, n), lax.rem(me + n - 1, n))
    rows, depth = x_ref.shape
    ff = wg_ref.shape[1]
    half = rows // 2
    group = n * half
    piece, strip = depth // PIECES, depth // STRIPS
    far, near = n // 2, n - 1 - n // 2
    hops = ((far, near), (near, far))
    up_tiles, down_tiles = ff // LANES, depth // (2 * WIDE)
    per_strip = down_tiles // STRIPS

    def at(offset):
        return lax.rem(me + offset + 2 * n, n)

    def upstream(way, k):
        return at(-k) if way == 0 else at(k)

    def downstream(way, k):
        return at(k) if way == 0 else at(-k)


    def gather_copy(h, way, chunk, p, a):
        span = pl.ds(pl.multiple_of(h * group + chunk * half, 16), half)
        wide = pl.ds(pl.multiple_of(p * piece, LANES), piece)
        index = a if h == 0 else a + hops[0][way] * PIECES
        return pltpu.make_async_remote_copy(
            src_ref=xg.at[span, wide],
            dst_ref=xg.at[span, wide],
            send_sem=ag_send.at[h, way],
            recv_sem=ag_recv.at[way, index],
            device_id={"tp": peer[way]},
            device_id_type=MESH,
        )

    def gather_own(h, way):
        def send(p, _):
            gather_copy(h, way, me, p, p).start()
            return 0

        lax.fori_loop(0, PIECES, send, 0)

    def gather_event(h, way, a, forward):
        hop = lax.div(a, PIECES)
        p = a - hop * PIECES
        chunk = upstream(way, hop + 1)
        gather_copy(h, way, chunk, p, a).wait_recv()
        if forward:
            gather_copy(h, way, chunk, p, a + PIECES).start()

    def gather_sent(h, way):
        span = pl.ds(0, hops[h][way] * half)
        pltpu.make_async_remote_copy(
            src_ref=xg.at[span],
            dst_ref=xg.at[span],
            send_sem=ag_send.at[h, way],
            recv_sem=ag_recv.at[way, 0],
            device_id={"tp": peer[way]},
            device_id_type=MESH,
        ).wait_send()


    def columns(p):
        return pl.ds(pl.multiple_of(p * strip, LANES), strip)

    def of_device(d):
        return pl.ds(pl.multiple_of(d * half, 16), half)

    def box(h, way, k, p):
        first = 0 if way == 0 else hops[h][0]
        span = pl.ds(pl.multiple_of((first + k - 1) * half, 16), half)
        return (slots if h == 0 else xg).at[span, columns(p)]

    def sum_copy(h, way, k, p, src, send_sem):
        return pltpu.make_async_remote_copy(
            src_ref=src,
            dst_ref=box(h, way, k, p),
            send_sem=send_sem,
            recv_sem=rs_recv.at[h, way, (k - 1) * STRIPS + p],
            device_id={"tp": peer[way]},
            device_id_type=MESH,
        )

    def sum_wait(h, way, k, p):
        arrived = box(h, way, k, p)
        sum_copy(h, way, k, p, arrived, rs_send.at[h, way]).wait_recv()
        return arrived

    def sum_head(h, p):
        for way in range(2):
            target = downstream(way, hops[h][way])
            held = stage.at[pl.ds(way * half, half), columns(p)]
            held[...] = terms[of_device(target), columns(p)].astype(jnp.bfloat16)
            sum_copy(h, way, 1, p, held, head_send.at[h, way]).start()

    def sum_event(h, way, e):
        hop = lax.div(e, STRIPS)
        p = e - hop * STRIPS
        arrived = sum_wait(h, way, hop + 1, p)
        target = downstream(way, hops[h][way] - 1 - hop)
        term = terms[of_device(target), columns(p)]
        arrived[...] = (arrived[...].astype(jnp.float32) + term).astype(jnp.bfloat16)
        sum_copy(h, way, hop + 2, p, arrived, rs_send.at[h, way]).start()

    def sums_sent(sem, ref, count):
        span = pl.ds(0, count)
        pltpu.make_async_remote_copy(
            src_ref=ref.at[span],
            dst_ref=ref.at[span],
            send_sem=sem,
            recv_sem=rs_recv.at[0, 0, 0],
            device_id={"tp": peer[0]},
            device_id_type=MESH,
        ).wait_send()


    def up_copies(i, s):
        span = pl.ds(pl.multiple_of(i * LANES, LANES), LANES)
        return [
            pltpu.make_async_copy(
                ref.at[:, span], wbuf.at[s, :, pl.ds(b * LANES, LANES)], w_sem.at[s, b]
            )
            for b, ref in enumerate((wg_ref, wu_ref))
        ]

    def down_copies(j, s):
        copies = []
        for b in range(2):
            span = pl.ds(pl.multiple_of((2 * j + b) * WIDE, WIDE), WIDE)
            copies.append(
                pltpu.make_async_copy(
                    wd_ref.at[:, span], wbuf.at[s, pl.ds(b * ff, ff)], w_sem.at[s, b]
                )
            )
        return copies

    def start(copies):
        for copy in copies:
            copy.start()

    def wait(copies):
        for copy in copies:
            copy.wait()

    def gate_up(h, first, events):
        def tile(i, _):
            s = lax.rem(first + i, 2)

            @pl.when(i + 1 < up_tiles)
            def _():
                start(up_copies(i + 1, 1 - s))

            @pl.when(i + 1 == up_tiles)
            def _():
                start(down_copies(0, 1 - s))

            wait(up_copies(i, s))
            both = jnp.dot(
                xg[h * group : (h + 1) * group, :],
                wbuf[s],
                preferred_element_type=jnp.float32,
            )
            gate, up = both[:, :LANES], both[:, LANES:]
            span = pl.ds(pl.multiple_of(i * LANES, LANES), LANES)
            hid[:, span] = (jax.nn.silu(gate) * up).astype(jnp.bfloat16)
            events(i)
            return 0

        lax.fori_loop(0, up_tiles, tile, 0)

    def down(h, first, before, after):
        def one_strip(p, _):
            before(p)

            def tile(t, _):
                j = p * per_strip + t
                s = lax.rem(first + j, 2)

                @pl.when(j + 1 < down_tiles)
                def _():
                    start(down_copies(j + 1, 1 - s))

                if h == 0:

                    @pl.when(j + 1 == down_tiles)
                    def _():
                        start(up_copies(0, 1 - s))

                wait(down_copies(j, s))
                for b in range(2):
                    span = pl.ds(pl.multiple_of((2 * j + b) * WIDE, WIDE), WIDE)
                    terms[:, span] = jnp.dot(
                        hid[...],
                        wbuf[s, b * ff : (b + 1) * ff, :],
                        preferred_element_type=jnp.float32,
                    )
                return 0

            lax.fori_loop(0, per_strip, tile, 0)
            after(p)
            return 0

        lax.fori_loop(0, STRIPS, one_strip, 0)

    def spread(i, tiles, delay, count, event):
        def upto(t):
            return lax.div(jnp.maximum(t - delay, 0) * count, tiles - delay)

        def run(e, _):
            event(e)
            return 0

        lax.fori_loop(upto(i), upto(i + 1), run, 0)

    def loop(lo, hi, event):
        def run(e, _):
            event(e)
            return 0

        lax.fori_loop(lo, hi, run, 0)


    own_copies = [
        pltpu.make_async_copy(
            x_ref.at[pl.ds(h * half, half)],
            xg.at[pl.ds(pl.multiple_of(h * group + me * half, 16), half)],
            x_sem.at[h],
        )
        for h in range(2)
    ]
    own_copies[0].start()

    barrier = pltpu.get_barrier_semaphore()
    for other in peer:
        pl.semaphore_signal(barrier, inc=1, device_id={"tp": other}, device_id_type=MESH)
    pl.semaphore_wait(barrier, 2)

    own_copies[0].wait()
    gather_own(0, 0)
    gather_own(0, 1)
    own_copies[1].start()
    start(up_copies(0, 0))
    own_copies[1].wait()

    def both_on(a):
        gather_event(0, 0, a, True)
        gather_event(0, 1, a, True)

    loop(0, (near - 1) * PIECES, both_on)
    gather_own(1, 1)

    def one_on(a):
        gather_event(0, 0, a, True)
        gather_event(0, 1, a, False)

    loop((near - 1) * PIECES, near * PIECES, one_on)
    gather_own(1, 0)

    def last_of_first(a):
        gather_event(0, 0, a, False)
        gather_event(1, 1, a - near * PIECES, True)

    loop(near * PIECES, far * PIECES, last_of_first)

    def second_on(j):
        gather_event(1, 0, j, True)
        gather_event(1, 1, j + PIECES, True)

    gate_up(
        0, 0,
        lambda i: spread(i, up_tiles, 0, (near - 1) * PIECES, second_on),
    )
    gather_sent(0, 0)
    gather_sent(0, 1)
    down(0, up_tiles, lambda p: None, lambda p: sum_head(0, p))

    def second_in(j):
        gather_event(1, 0, j, False)
        gather_event(1, 1, j + PIECES, False)

    loop((near - 1) * PIECES, near * PIECES, second_in)

    def first_sums(e):
        sum_event(0, 0, e)
        sum_event(0, 1, e)

    gate_up(
        1, up_tiles + down_tiles,
        lambda i: spread(i, up_tiles, min(DELAY, up_tiles - 1), (near - 1) * STRIPS, first_sums),
    )
    for way in range(2):
        sums_sent(head_send.at[0, way], stage, half)

    def near_end(p):
        sum_event(0, 0, (near - 1) * STRIPS + p)
        arrived = sum_wait(0, 1, near, p)
        own[:, columns(p)] = arrived[...].astype(jnp.float32) + terms[of_device(me), columns(p)]

    down(1, 2 * up_tiles + down_tiles, near_end, lambda p: sum_head(1, p))

    def first_end(p):
        arrived = sum_wait(0, 0, far, p)
        total = arrived[...].astype(jnp.float32) + own[:, columns(p)]
        y_ref[pl.ds(0, half), columns(p)] = total.astype(jnp.bfloat16)
        sum_event(1, 1, p)

    loop(0, STRIPS, first_end)

    def second_sums(e):
        sum_event(1, 1, e + STRIPS)
        sum_event(1, 0, e)

    loop(0, (near - 1) * STRIPS, second_sums)

    def second_end(p):
        one, other = sum_wait(1, 0, near, p), sum_wait(1, 1, far, p)
        total = one[...].astype(jnp.float32) + other[...].astype(jnp.float32)
        total += terms[of_device(me), columns(p)]
        y_ref[pl.ds(half, half), columns(p)] = total.astype(jnp.bfloat16)

    loop(0, STRIPS, second_end)

    for way in range(2):
        gather_sent(1, way)
        sums_sent(head_send.at[1, way], stage, half)
        for h in range(2):
            sums_sent(rs_send.at[h, way], slots, (hops[h][way] - 1) * half)


def solution(mesh):
    n = mesh.shape["tp"]

    def step(x, w_gate, w_up, w_down):
        rows, depth = x.shape
        ff = w_gate.shape[1]
        half = rows // 2
        far = n // 2
        bf16, f32 = jnp.bfloat16, jnp.float32
        dma = pltpu.SemaphoreType.DMA
        return pl.pallas_call(
            functools.partial(kernel, n),
            name="mlp_ring",
            out_shape=pltpu.VMEM((rows, depth), x.dtype),
            in_specs=[pl.BlockSpec(memory_space=pl.ANY)] * 4,
            out_specs=pl.BlockSpec(memory_space=pltpu.VMEM),
            scratch_shapes=[
                pltpu.VMEM((n * rows, depth), bf16),
                pltpu.VMEM((n * half, ff), bf16),
                pltpu.VMEM((n * half, depth), f32),
                pltpu.VMEM((2, depth, WIDE), bf16),
                pltpu.VMEM(((n - 1) * half, depth), bf16),
                pltpu.VMEM((2 * half, depth), bf16),
                pltpu.VMEM((half, depth), f32),
                dma((2,)),
                dma((2, 2)),
                dma((2, 2)),
                dma((2, (n - 1) * PIECES)),
                dma((2, 2)),
                dma((2, 2)),
                dma((2, 2, far * STRIPS)),
            ],
            compiler_params=pltpu.CompilerParams(
                collective_id=0, has_side_effects=True, vmem_limit_bytes=VMEM_GRANT
            ),
        )(x, w_gate, w_up, w_down)

    return jax.shard_map(
        step,
        mesh=mesh,
        in_specs=(P(("dp", "tp"), None), P(None, "tp"), P(None, "tp"), P("tp", None)),
        out_specs=P(("dp", "tp"), None),
        check_vma=False,
    )
```
